32 devices in a mesh: row: 16 (over z, x, core), col: 2 (over y).
Axes of the slice: x: 2, y: 2, z: 4, core: 2. Of those that a mesh axis runs over, the one named last changes fastest.
Arguments:
- features: bfloat16 [4096, 440], P(('row', 'col')), may hold values from -1 to 1
- coeffs: bfloat16 [4096, 144], P(('row', 'col')), may hold values from -0.375 to 0.375
- targets: float32 [4096, 144], P(('row', 'col')), may hold values from -6 to 6
Outputs:
- residual: float32 [4096, 144], P(('row', 'col'))
The draws below stay inside these ranges and needn't reach their ends.
All inputs are finite; a program needn't handle non-finite values.
Results may differ from the reference program's by a relative error of at most 0.0012.
Values may be sent and summed in bfloat16 or wider, within the bound.
No kernel may reach another device: no remote copies, remote signals or barrier semaphores. Data moves between devices by JAX's collectives and lax.ppermute only.
A program may use at most 64 MiB of HBM per device.

```python
import math
import jax
import jax.numpy as jnp
from jax import lax

FEAT = 440
OUTS = 144
FRAMES = 4096


def draw_features(key, part):
    clusters = math.gcd(32, FRAMES)
    members = FRAMES // clusters
    streams = jax.random.split(jax.random.fold_in(key, 7301), 7)
    centre_basis = jax.random.normal(streams[0], (8, FEAT), jnp.float32) / math.sqrt(FEAT)
    local_basis = jax.random.normal(streams[1], (clusters, 16, FEAT), jnp.float32) / math.sqrt(FEAT)
    centre_coords = jax.random.normal(streams[2], (clusters, 8), jnp.float32) * 0.9
    spread = jnp.exp(jax.random.uniform(streams[3], (clusters, 1, 1), jnp.float32, math.log(0.04), math.log(0.3)))
    latent = jax.random.normal(streams[4], (clusters, members, 16), jnp.float32) * spread
    noise = jax.random.normal(streams[5], (clusters, members, FEAT), jnp.float32) * 0.01
    centres = jnp.dot(centre_coords, centre_basis)
    local = jnp.einsum('cmk,ckf->cmf', latent, local_basis)
    frames = (centres[:, None, :] + local + noise).reshape(FRAMES, FEAT)
    order = jax.random.permutation(streams[6], FRAMES)
    frames = frames[order]
    return jnp.clip(frames, -1.0, 1.0).astype(jnp.bfloat16)


def level_of(own_key, extent, pieces, least, high):
    level = 1.0
    for axis_at, shards_of in pieces:
        draws = jax.random.uniform(jax.random.fold_in(jax.random.fold_in(own_key, 6), axis_at), (shards_of,), jnp.float32, least / len(pieces), high / len(pieces))
        level = level * jnp.repeat(jnp.exp(draws), extent[axis_at] // shards_of).reshape((-1,) + (1,) * (len(extent) - 1 - axis_at))
    return level


def normal_values(own_key, extent, width, most, shards=(), held_as=jnp.bfloat16):
    result = jax.random.normal(own_key, extent, jnp.float32) * width
    if len(shards) > 0:
        result = level_of(own_key, extent, shards, -0.22, 0.18) * result
    return jnp.clip(result, min=-most, max=most).astype(held_as)


def setup_inputs(seed: int = 0) -> dict:
    key_list = jax.random.split(jax.random.key(seed), 4)
    return {
        "features": draw_features(jax.random.fold_in(key_list[3], 71), 0),
        "coeffs": normal_values(key_list[1], (FRAMES, OUTS), (FRAMES // 16) ** -0.5, 0.375, ((0, 32),)),
        "targets": normal_values(key_list[2], (FRAMES, OUTS), 1.0, 6.0, ((0, 32),), jnp.float32),
    }


def reference(features, coeffs, targets):
    whole = features.astype(jnp.float32)
    sq = lax.optimization_barrier(jnp.sum(whole * whole, axis=1))
    weights = coeffs.astype(jnp.float32)
    blocks = FRAMES // 1024 if FRAMES % 1024 == 0 else 1
    size = FRAMES // blocks

    def one_block(index):
        start = (index * size).astype(jnp.int32)
        query = lax.dynamic_slice_in_dim(whole, start, size, 0)
        query_sq = lax.dynamic_slice_in_dim(sq, start, size, 0)
        inner = jnp.dot(query, whole.T, precision=lax.Precision.HIGHEST)
        dist = jnp.sqrt(jnp.maximum(query_sq[:, None] + sq[None, :] - 2.0 * inner, 0.0))
        kernel = jnp.exp(-dist).astype(jnp.bfloat16).astype(jnp.float32)
        return jnp.dot(kernel, weights, precision=lax.Precision.HIGHEST)
    parts = lax.map(one_block, jnp.arange(blocks, dtype=jnp.int32))
    return parts.reshape(FRAMES, OUTS) - targets
```

```python
import functools
import math

import jax
import jax.numpy as jnp
from jax import lax
from jax.experimental import pallas as pl
from jax.experimental.pallas import tpu as pltpu
from jax.sharding import PartitionSpec as P

AXES = ("row", "col")
NEAR_BYTES = 2 << 20
LOG2E = math.log2(math.e)


def kernel_products(queries, keys, weights):
    nq, nk = len(queries), len(keys)
    outs = weights[0].shape[0]
    step = 2 if nk % 2 == 0 else 1

    def body(*refs):
        q_refs, k_refs, w_refs = refs[:nq], refs[nq:nq + nk], refs[nq + nk:nq + 2 * nk]
        out_refs = refs[nq + 2 * nk:]
        lhs, lhs_sq = [], []
        for q_ref in q_refs:
            q = q_ref[...].T
            q32 = q.astype(jnp.float32)
            lhs.append((q32 * -2.0).astype(jnp.bfloat16))
            lhs_sq.append(jnp.sum(q32 * q32, axis=1, keepdims=True))
        acc = [None] * nq
        for k in range(0, nk, step):
            rhs = jnp.concatenate([k_refs[k + s][...] for s in range(step)], axis=1)
            w = jnp.concatenate([w_refs[k + s][...] for s in range(step)], axis=1)
            rhs32 = rhs.astype(jnp.float32)
            rhs_sq = jnp.sum(rhs32 * rhs32, axis=0, keepdims=True)
            for i in range(nq):
                inner = jnp.dot(lhs[i], rhs, preferred_element_type=jnp.float32)
                d2 = jnp.maximum((inner + rhs_sq) + lhs_sq[i], 1e-30)
                kern = jnp.exp2((d2 * -LOG2E) * lax.rsqrt(d2)).astype(jnp.bfloat16)
                part = lax.dot_general(
                    w, kern, (((1,), (1,)), ((), ())), preferred_element_type=jnp.float32
                )
                acc[i] = part if acc[i] is None else acc[i] + part
        for i in range(nq):
            out_refs[i][...] = acc[i].astype(out_refs[i].dtype)

    held = [*queries, *keys, *weights]
    shapes = [
        ((outs, q.shape[1]), jnp.float32 if i == 0 else jnp.bfloat16)
        for i, q in enumerate(queries)
    ]
    vmem = pl.BlockSpec(memory_space=pltpu.VMEM)
    if sum(a.size * a.dtype.itemsize for a in held) <= NEAR_BYTES:
        held = [pltpu.with_memory_space_constraint(a, pltpu.VMEM) for a in held]
        shapes = [pltpu.VMEM(*s) for s in shapes]
    else:
        shapes = [jax.ShapeDtypeStruct(*s) for s in shapes]
    return pl.pallas_call(
        body,
        out_shape=shapes,
        in_specs=[vmem] * (nq + 2 * nk),
        out_specs=[vmem] * nq,
        name="products",
    )(*held)


def per_device(rows, cols, features, coeffs, targets):
    total = rows * cols
    core, xbit, z = cols, 2 * cols, 4 * cols

    def swap(value, bits):
        return lax.ppermute(value, AXES, [(i, i ^ bits) for i in range(total)])

    mine = features.T
    coef = coeffs.T
    queries = [mine]
    order = [0]
    bit = rows // 8
    while bit >= 1:
        queries = queries + [swap(q, bit * z) for q in queries]
        order = order + [o ^ (bit * z) for o in order]
        bit = bit // 2
    keys, weights = [mine], [coef]
    for plane in range(1, 2 * cols):
        bits = (plane // cols) * xbit + plane % cols
        keys.append(swap(mine, bits))
        weights.append(swap(coef, bits))
    keys = keys + [swap(k, core) for k in keys]
    weights = weights + [swap(w, core) for w in weights]

    parts = kernel_products(queries, keys, weights)
    total_part = parts[0] - targets.T
    for bits, part in list(zip(order, parts))[1:]:
        total_part = total_part + swap(part, bits).astype(jnp.float32)
    return total_part.T


def solution(mesh):
    body = functools.partial(per_device, mesh.shape["row"], mesh.shape["col"])
    spec = P(AXES, None)
    return jax.shard_map(
        body, mesh=mesh, in_specs=(spec, spec, spec), out_specs=spec, check_vma=False
    )
```

```python
import functools
import math

import jax
import jax.numpy as jnp
from jax import lax
from jax.experimental import pallas as pl
from jax.experimental.pallas import tpu as pltpu
from jax.sharding import PartitionSpec as P

AXES = ("row", "col")
NEAR_BYTES = 2 << 20
LOG2E = math.log2(math.e)


def square_rows(wide, shift):
    sq = jnp.sum(wide * wide, axis=0, keepdims=True)
    high = sq.astype(jnp.bfloat16).astype(jnp.float32)
    mid = (sq - high).astype(jnp.bfloat16).astype(jnp.float32)
    low = (sq - high) - mid
    row = lax.broadcasted_iota(jnp.int32, (8, wide.shape[1]), 0)
    rest = jnp.where(row < 6, 1.0, 0.0)
    for n, part in enumerate((high, mid, low)):
        rest = jnp.where(row == shift + n, part, rest)
    return rest.astype(jnp.bfloat16)


def stacked(weights, values, near):
    outs, feats, width = weights.shape[0], values.shape[0], values.shape[1]

    def body(weight_ref, value_ref, out_ref):
        out_ref[:outs, :] = weight_ref[...]
        value = value_ref[...]
        out_ref[outs:outs + feats, :] = value
        out_ref[outs + feats:, :] = square_rows(value.astype(jnp.float32), 0)

    shape = (outs + feats + 8, width)
    vmem = pl.BlockSpec(memory_space=pltpu.VMEM)
    return pl.pallas_call(
        body,
        out_shape=pltpu.VMEM(shape, values.dtype) if near else jax.ShapeDtypeStruct(shape, values.dtype),
        in_specs=[vmem] * 2,
        out_specs=vmem,
        name="stacked",
    )(weights, values)


def products(work, outs, feats, kinds, near):
    arrays, slots = [], {}

    def slot(a):
        if id(a) not in slots:
            slots[id(a)] = len(arrays)
            arrays.append(a)
        return slots[id(a)]

    plan = [
        (slot(q), [slot(k) for k in keys], None if old is None else slot(old))
        for q, keys, old in work
    ]
    count = len(arrays)
    width = work[0][0].shape[1]

    def body(*refs):
        ins, out_refs, left_ref = refs[:count], refs[count:-1], refs[-1]
        for n, (q, _, _) in enumerate(plan):
            skip = outs if ins[q].shape[0] > feats else 0
            value = ins[q][skip:skip + feats, :]
            wide = value.astype(jnp.float32)
            left_ref[n, :feats, :] = (wide * -2.0).astype(jnp.bfloat16)
            left_ref[n, feats:, :] = square_rows(wide, 3)
        lhs = [left_ref[n].T for n in range(len(plan))]
        acc = [None if old is None else ins[old][...] for _, _, old in plan]
        groups = []
        for _, keys, _ in plan:
            for n in range(0, len(keys), 2):
                group = tuple(keys[n:n + 2])
                if group not in groups:
                    groups.append(group)
        for group in groups:
            rhs = jnp.concatenate([ins[k][outs:, :] for k in group], axis=1)
            weight = jnp.concatenate([ins[k][:outs, :] for k in group], axis=1)
            users = [i for i, (_, keys, _) in enumerate(plan) if group[0] in keys]
            left = jnp.concatenate([lhs[i] for i in users], axis=0)
            d2 = jnp.maximum(jnp.dot(left, rhs, preferred_element_type=jnp.float32), 1e-30)
            kern = jnp.exp2((d2 * -LOG2E) * lax.rsqrt(d2)).astype(jnp.bfloat16)
            part = lax.dot_general(
                weight, kern, (((1,), (1,)), ((), ())), preferred_element_type=jnp.float32
            )
            for n, i in enumerate(users):
                mine = part[:, n * width:(n + 1) * width]
                acc[i] = mine if acc[i] is None else acc[i] + mine
        for i in range(len(plan)):
            out_refs[i][...] = acc[i].astype(out_refs[i].dtype)

    shapes = [((outs, width), kind) for kind in kinds]
    vmem = pl.BlockSpec(memory_space=pltpu.VMEM)
    if near:
        arrays = [pltpu.with_memory_space_constraint(a, pltpu.VMEM) for a in arrays]
        shapes = [pltpu.VMEM(*s) for s in shapes]
    else:
        shapes = [jax.ShapeDtypeStruct(*s) for s in shapes]
    return pl.pallas_call(
        body,
        out_shape=shapes,
        in_specs=[vmem] * count,
        out_specs=[vmem] * len(work),
        scratch_shapes=[pltpu.VMEM((len(work), feats + 8, width), jnp.bfloat16)],
        name="products",
    )(*arrays)


def per_device(rows, cols, features, coeffs, targets):
    total = rows * cols
    core, xbit, z = cols, 2 * cols, 4 * cols
    f32, b16 = jnp.float32, jnp.bfloat16

    def swap(value, bits):
        return lax.ppermute(value, AXES, [(i, i ^ bits) for i in range(total)])

    mine = features.T
    outs = coeffs.shape[1]
    queries, order = [mine], [0]
    bit = rows // 8
    while bit >= 1:
        bits = bit * z
        queries = queries + [swap(q, bits) for q in queries]
        order = order + [o ^ bits for o in order]
        bit = bit // 2
    near = sum(a.size * a.dtype.itemsize for a in queries) * 8 <= NEAR_BYTES * 2
    both = stacked(coeffs.T, mine, near)
    queries[0] = both
    blocks = [both]
    for plane in reversed(range(1, 2 * cols)):
        bits = (plane // cols) * xbit + plane % cols
        blocks.append(swap(both, bits))
    keys = []
    for b in blocks:
        keys = keys + [b, swap(b, core)]

    feats = mine.shape[0]
    half = len(keys) // 2
    lead = queries[:-1] if len(queries) > 1 else queries
    early = products([(q, keys[:half], None) for q in lead], outs, feats, [f32] * len(lead), near)
    sent = [(q, keys[half:], e) for q, e in zip(lead, early)][1:]
    sent = sent + [(q, keys, None) for q in queries[len(lead):]]
    parts = products(sent, outs, feats, [b16] * len(sent), near) if sent else []
    own = products([(queries[0], keys[half:], early[0])], outs, feats, [f32], near)[0]
    result = own - targets.T
    for n, part in enumerate(parts):
        result = result + swap(part, order[n + 1]).astype(f32)
    return result.T


def solution(mesh):
    rows, cols = mesh.shape["row"], mesh.shape["col"]
    spec = P(AXES, None)
    body = functools.partial(per_device, rows, cols)
    return jax.shard_map(
        body, mesh=mesh, in_specs=(spec, spec, spec), out_specs=spec, check_vma=False
    )
```

```python
import functools
import math

import jax
import jax.numpy as jnp
from jax import lax
from jax.experimental import pallas as pl
from jax.experimental.pallas import tpu as pltpu
from jax.sharding import PartitionSpec as P

AXES = ("row", "col")
NEAR_BYTES = 2 << 20
LOG2E = math.log2(math.e)


def square_rows(wide, shift):
    sq = jnp.sum(wide * wide, axis=0, keepdims=True)
    high = sq.astype(jnp.bfloat16).astype(jnp.float32)
    mid = (sq - high).astype(jnp.bfloat16).astype(jnp.float32)
    low = (sq - high) - mid
    row = lax.broadcasted_iota(jnp.int32, (8, wide.shape[1]), 0)
    rest = jnp.where(row < 6, 1.0, 0.0)
    for n, part in enumerate((high, mid, low)):
        rest = jnp.where(row == shift + n, part, rest)
    return rest.astype(jnp.bfloat16)


def stacked(weights, values, near):
    outs, feats, width = weights.shape[0], values.shape[0], values.shape[1]

    def body(weight_ref, value_ref, out_ref):
        out_ref[:outs, :] = weight_ref[...]
        value = value_ref[...]
        out_ref[outs:outs + feats, :] = value
        out_ref[outs + feats:, :] = square_rows(value.astype(jnp.float32), 0)

    shape = (outs + feats + 8, width)
    vmem = pl.BlockSpec(memory_space=pltpu.VMEM)
    return pl.pallas_call(
        body,
        out_shape=pltpu.VMEM(shape, values.dtype) if near else jax.ShapeDtypeStruct(shape, values.dtype),
        in_specs=[vmem] * 2,
        out_specs=vmem,
        name="stacked",
    )(weights, values)


def products(work, outs, feats, kinds, near):
    arrays, slots = [], {}

    def slot(a):
        if id(a) not in slots:
            slots[id(a)] = len(arrays)
            arrays.append(a)
        return slots[id(a)]

    plan = [
        (slot(q), [slot(k) for k in keys], None if old is None else slot(old))
        for q, keys, old in work
    ]
    count = len(arrays)
    width = work[0][0].shape[1]

    def body(*refs):
        ins, out_refs, left_ref = refs[:count], refs[count:-1], refs[-1]
        for n, (q, _, _) in enumerate(plan):
            skip = outs if ins[q].shape[0] > feats else 0
            value = ins[q][skip:skip + feats, :]
            wide = value.astype(jnp.float32)
            left_ref[n, :feats, :] = (wide * -2.0).astype(jnp.bfloat16)
            left_ref[n, feats:, :] = square_rows(wide, 3)
        lhs = [left_ref[n].T for n in range(len(plan))]
        acc = [None for _ in plan]
        groups = []
        for _, keys, _ in plan:
            for n in range(0, len(keys), 2):
                group = tuple(keys[n:n + 2])
                if group not in groups:
                    groups.append(group)
        for group in groups:
            rhs = jnp.concatenate([ins[k][outs:, :] for k in group], axis=1)
            weight = jnp.concatenate([ins[k][:outs, :] for k in group], axis=1)
            users = [i for i, (_, keys, _) in enumerate(plan) if group[0] in keys]
            left = jnp.concatenate([lhs[i] for i in users], axis=0)
            d2 = jnp.maximum(jnp.dot(left, rhs, preferred_element_type=jnp.float32), 1e-30)
            kern = jnp.exp2((d2 * -LOG2E) * lax.rsqrt(d2)).astype(jnp.bfloat16)
            part = lax.dot_general(
                kern, weight, (((1,), (1,)), ((), ())), preferred_element_type=jnp.float32
            )
            for n, i in enumerate(users):
                mine = part[n * width:(n + 1) * width, :]
                acc[i] = mine if acc[i] is None else acc[i] + mine
        for i in range(len(plan)):
            total = acc[i].T
            old = plan[i][2]
            total = total if old is None else total + ins[old][...]
            out_refs[i][...] = total.astype(out_refs[i].dtype)

    shapes = [((outs, width), kind) for kind in kinds]
    vmem = pl.BlockSpec(memory_space=pltpu.VMEM)
    if near:
        arrays = [pltpu.with_memory_space_constraint(a, pltpu.VMEM) for a in arrays]
        shapes = [pltpu.VMEM(*s) for s in shapes]
    else:
        shapes = [jax.ShapeDtypeStruct(*s) for s in shapes]
    return pl.pallas_call(
        body,
        out_shape=shapes,
        in_specs=[vmem] * count,
        out_specs=[vmem] * len(work),
        scratch_shapes=[pltpu.VMEM((len(work), feats + 8, width), jnp.bfloat16)],
        name="products",
    )(*arrays)


def per_device(rows, cols, features, coeffs, targets):
    total = rows * cols
    core, xbit, z = cols, 2 * cols, 4 * cols
    f32, b16 = jnp.float32, jnp.bfloat16

    def swap(value, bits):
        return lax.ppermute(value, AXES, [(i, i ^ bits) for i in range(total)])

    mine = features.T
    outs = coeffs.shape[1]
    queries, order = [mine], [0]
    bit = rows // 8
    while bit >= 1:
        bits = bit * z
        queries = queries + [swap(q, bits) for q in queries]
        order = order + [o ^ bits for o in order]
        bit = bit // 2
    near = sum(a.size * a.dtype.itemsize for a in queries) * 8 <= NEAR_BYTES * 2
    both = stacked(coeffs.T, mine, near)
    queries[0] = both
    blocks = [both]
    for plane in reversed(range(1, 2 * cols)):
        bits = (plane // cols) * xbit + plane % cols
        blocks.append(swap(both, bits))
    keys = []
    for b in blocks:
        keys = keys + [b, swap(b, core)]

    feats = mine.shape[0]
    half = len(keys) // 2
    lead = queries[:-1] if len(queries) > 1 else queries
    early = products([(q, keys[:half], None) for q in lead], outs, feats, [f32] * len(lead), near)
    sent = [(q, keys[half:], e) for q, e in zip(lead, early)][1:]
    sent = sent + [(q, keys, None) for q in queries[len(lead):]]
    parts = products(sent, outs, feats, [b16] * len(sent), near) if sent else []
    own = products([(queries[0], keys[half:], early[0])], outs, feats, [f32], near)[0]
    result = own - targets.T
    for n, part in enumerate(parts):
        result = result + swap(part, order[n + 1]).astype(f32)
    return result.T


def solution(mesh):
    rows, cols = mesh.shape["row"], mesh.shape["col"]
    spec = P(AXES, None)
    body = functools.partial(per_device, rows, cols)
    return jax.shard_map(
        body, mesh=mesh, in_specs=(spec, spec, spec), out_specs=spec, check_vma=False
    )
```

```python
import functools
import math

import jax
import jax.numpy as jnp
from jax import lax
from jax.experimental import pallas as pl
from jax.experimental.pallas import tpu as pltpu
from jax.sharding import PartitionSpec as P

AXES = ("row", "col")
NEAR_BYTES = 2 << 20
LOG2E = math.log2(math.e)


def square_rows(wide, shift):
    sq = jnp.sum(wide * wide, axis=0, keepdims=True)
    high = sq.astype(jnp.bfloat16).astype(jnp.float32)
    mid = (sq - high).astype(jnp.bfloat16).astype(jnp.float32)
    low = (sq - high) - mid
    row = lax.broadcasted_iota(jnp.int32, (8, wide.shape[1]), 0)
    rest = jnp.where(row < 6, 1.0, 0.0)
    for n, part in enumerate((high, mid, low)):
        rest = jnp.where(row == shift + n, part, rest)
    return rest.astype(jnp.bfloat16)


def stacked(weights, values, near):
    outs, feats, width = weights.shape[0], values.shape[0], values.shape[1]

    def body(weight_ref, value_ref, out_ref):
        out_ref[:outs, :] = weight_ref[...]
        value = value_ref[...]
        out_ref[outs:outs + feats, :] = value
        out_ref[outs + feats:, :] = square_rows(value.astype(jnp.float32), 0)

    shape = (outs + feats + 8, width)
    vmem = pl.BlockSpec(memory_space=pltpu.VMEM)
    return pl.pallas_call(
        body,
        out_shape=pltpu.VMEM(shape, values.dtype) if near else jax.ShapeDtypeStruct(shape, values.dtype),
        in_specs=[vmem] * 2,
        out_specs=vmem,
        name="stacked",
    )(weights, values)


def products(work, outs, feats, kinds, near, prepared=0):
    arrays, slots = [], {}

    def slot(a):
        if id(a) not in slots:
            slots[id(a)] = len(arrays)
            arrays.append(a)
        return slots[id(a)]

    plan = [
        (
            slot(q[0] if isinstance(q, tuple) else q),
            isinstance(q, tuple),
            [slot(k) for k in keys],
            None if old is None else slot(old),
        )
        for q, keys, old in work
    ]
    count, entries = len(arrays), len(work)
    width = work[0][1][0].shape[1]

    def body(*refs):
        ins, out_refs, left_ref = refs[:count], refs[count:-1], refs[-1]
        lhs = []
        for n, (q, ready, _, _) in enumerate(plan):
            if ready:
                lhs.append(ins[q][...])
                continue
            skip = outs if ins[q].shape[0] > feats else 0
            wide = ins[q][skip:skip + feats, :].astype(jnp.float32)
            left_ref[n, :feats, :] = (wide * -2.0).astype(jnp.bfloat16)
            left_ref[n, feats:, :] = square_rows(wide, 3)
            lhs.append(left_ref[n].T)
        for n in range(prepared):
            out_refs[entries + n][...] = lhs[entries - prepared + n]
        acc = [None for _ in plan]
        groups = []
        for _, _, keys, _ in plan:
            for n in range(0, len(keys), 2):
                group = tuple(keys[n:n + 2])
                if group not in groups:
                    groups.append(group)
        for group in groups:
            rhs = jnp.concatenate([ins[k][outs:, :] for k in group], axis=1)
            weight = jnp.concatenate([ins[k][:outs, :] for k in group], axis=1)
            users = [i for i, (_, _, keys, _) in enumerate(plan) if group[0] in keys]
            left = jnp.concatenate([lhs[i] for i in users], axis=0)
            d2 = jnp.maximum(jnp.dot(left, rhs, preferred_element_type=jnp.float32), 1e-30)
            kern = jnp.exp2((d2 * -LOG2E) * lax.rsqrt(d2)).astype(jnp.bfloat16)
            part = lax.dot_general(
                kern, weight, (((1,), (1,)), ((), ())), preferred_element_type=jnp.float32
            )
            for n, i in enumerate(users):
                mine = part[n * width:(n + 1) * width, :]
                acc[i] = mine if acc[i] is None else acc[i] + mine
        for i in range(entries):
            total = acc[i].T
            old = plan[i][3]
            total = total if old is None else total + ins[old][...]
            out_refs[i][...] = total.astype(out_refs[i].dtype)

    shapes = [((outs, width), kind) for kind in kinds]
    shapes = shapes + [((width, feats + 8), jnp.bfloat16)] * prepared
    vmem = pl.BlockSpec(memory_space=pltpu.VMEM)
    if near:
        arrays = [pltpu.with_memory_space_constraint(a, pltpu.VMEM) for a in arrays]
        shapes = [pltpu.VMEM(*s) for s in shapes]
    else:
        shapes = [jax.ShapeDtypeStruct(*s) for s in shapes]
    return pl.pallas_call(
        body,
        out_shape=shapes,
        in_specs=[vmem] * count,
        out_specs=[vmem] * len(shapes),
        scratch_shapes=[pltpu.VMEM((entries, feats + 8, width), jnp.bfloat16)],
        name="products",
    )(*arrays)


def per_device(rows, cols, features, coeffs, targets):
    total = rows * cols
    core, xbit, z = cols, 2 * cols, 4 * cols
    f32, b16 = jnp.float32, jnp.bfloat16

    def swap(value, bits):
        return lax.ppermute(value, AXES, [(i, i ^ bits) for i in range(total)])

    mine = features.T
    outs = coeffs.shape[1]
    queries, order = [mine], [0]
    bit = rows // 8
    while bit >= 1:
        bits = bit * z
        queries = queries + [swap(q, bits) for q in queries]
        order = order + [o ^ bits for o in order]
        bit = bit // 2
    near = sum(a.size * a.dtype.itemsize for a in queries) * 8 <= NEAR_BYTES * 2
    both = stacked(coeffs.T, mine, near)
    queries[0] = both
    blocks = [both]
    for plane in reversed(range(1, 2 * cols)):
        bits = (plane // cols) * xbit + plane % cols
        blocks.append(swap(both, bits))
    keys = []
    for b in blocks:
        keys = keys + [b, swap(b, core)]

    feats = mine.shape[0]
    half = len(keys) // 2
    lead = queries[:-1] if len(queries) > 1 else queries
    run = functools.partial(products, outs=outs, feats=feats, near=near)
    got = run([(q, keys[:half], None) for q in lead], kinds=[f32] * len(lead), prepared=len(lead))
    early, ready = got[:len(lead)], [(a,) for a in got[len(lead):]]
    sent = [(q, keys[half:], e) for q, e in zip(ready, early)][1:]
    sent = sent + [(q, keys, None) for q in queries[len(lead):]]
    parts = run(sent, kinds=[b16] * len(sent)) if sent else []
    own = run([(ready[0], keys[half:], early[0])], kinds=[f32])[0]
    result = own - targets.T
    for n, part in enumerate(parts):
        result = result + swap(part, order[n + 1]).astype(f32)
    return result.T


def solution(mesh):
    rows, cols = mesh.shape["row"], mesh.shape["col"]
    spec = P(AXES, None)
    body = functools.partial(per_device, rows, cols)
    return jax.shard_map(
        body, mesh=mesh, in_specs=(spec, spec, spec), out_specs=spec, check_vma=False
    )
```

```python
import functools
import math

import jax
import jax.numpy as jnp
from jax import lax
from jax.experimental import pallas as pl
from jax.experimental.pallas import tpu as pltpu
from jax.sharding import PartitionSpec as P

AXES = ("row", "col")
NEAR_BYTES = 2 << 20
LOG2E = math.log2(math.e)


def square_rows(wide, shift):
    sq = jnp.sum(wide * wide, axis=0, keepdims=True)
    high = sq.astype(jnp.bfloat16).astype(jnp.float32)
    mid = (sq - high).astype(jnp.bfloat16).astype(jnp.float32)
    low = (sq - high) - mid
    row = lax.broadcasted_iota(jnp.int32, (8, wide.shape[1]), 0)
    rest = jnp.where(row < 6, 1.0, 0.0)
    for n, part in enumerate((high, mid, low)):
        rest = jnp.where(row == shift + n, part, rest)
    return rest.astype(jnp.bfloat16)


def stacked(weights, values, near):
    outs, feats, width = weights.shape[0], values.shape[0], values.shape[1]

    def body(weight_ref, value_ref, out_ref):
        out_ref[:outs, :] = weight_ref[...]
        value = value_ref[...]
        out_ref[outs:outs + feats, :] = value
        out_ref[outs + feats:, :] = square_rows(value.astype(jnp.float32), 0)

    shape = (outs + feats + 8, width)
    vmem = pl.BlockSpec(memory_space=pltpu.VMEM)
    return pl.pallas_call(
        body,
        out_shape=pltpu.VMEM(shape, values.dtype) if near else jax.ShapeDtypeStruct(shape, values.dtype),
        in_specs=[vmem] * 2,
        out_specs=vmem,
        name="stacked",
    )(weights, values)


def products(work, outs, feats, kinds, near, prepared=0, minus=None):
    arrays, slots = [], {}

    def slot(a):
        if id(a) not in slots:
            slots[id(a)] = len(arrays)
            arrays.append(a)
        return slots[id(a)]

    plan = [
        (
            slot(q[0] if isinstance(q, tuple) else q),
            isinstance(q, tuple),
            [slot(k) for k in keys],
            None if old is None else slot(old),
        )
        for q, keys, old in work
    ]
    taken = None if minus is None else slot(minus)
    count, entries = len(arrays), len(work)
    width = work[0][1][0].shape[1]

    def body(*refs):
        ins, out_refs, left_ref = refs[:count], refs[count:-1], refs[-1]
        lhs = []
        for n, (q, ready, _, _) in enumerate(plan):
            if ready:
                lhs.append(ins[q][...])
                continue
            skip = outs if ins[q].shape[0] > feats else 0
            wide = ins[q][skip:skip + feats, :].astype(jnp.float32)
            left_ref[n, :feats, :] = (wide * -2.0).astype(jnp.bfloat16)
            left_ref[n, feats:, :] = square_rows(wide, 3)
            lhs.append(left_ref[n].T)
        for n in range(prepared):
            out_refs[entries + n][...] = lhs[entries - prepared + n]
        acc = [None for _ in plan]
        groups = []
        for _, _, keys, _ in plan:
            for n in range(0, len(keys), 2):
                group = tuple(keys[n:n + 2])
                if group not in groups:
                    groups.append(group)
        for group in groups:
            rhs = jnp.concatenate([ins[k][outs:, :] for k in group], axis=1)
            weight = jnp.concatenate([ins[k][:outs, :] for k in group], axis=1)
            users = [i for i, (_, _, keys, _) in enumerate(plan) if group[0] in keys]
            left = jnp.concatenate([lhs[i] for i in users], axis=0)
            d2 = jnp.maximum(jnp.dot(left, rhs, preferred_element_type=jnp.float32), 1e-30)
            kern = jnp.exp2((d2 * -LOG2E) * lax.rsqrt(d2)).astype(jnp.bfloat16)
            part = lax.dot_general(
                kern, weight, (((1,), (1,)), ((), ())), preferred_element_type=jnp.float32
            )
            for n, i in enumerate(users):
                mine = part[n * width:(n + 1) * width, :]
                acc[i] = mine if acc[i] is None else acc[i] + mine
        for i in range(entries):
            total = acc[i].T
            old = plan[i][3]
            total = total if old is None else total + ins[old][...]
            total = total if taken is None else total - ins[taken][...]
            out_refs[i][...] = total.astype(out_refs[i].dtype)

    shapes = [((outs, width), kind) for kind in kinds]
    shapes = shapes + [((width, feats + 8), jnp.bfloat16)] * prepared
    vmem = pl.BlockSpec(memory_space=pltpu.VMEM)
    if near:
        arrays = [pltpu.with_memory_space_constraint(a, pltpu.VMEM) for a in arrays]
        shapes = [pltpu.VMEM(*s) for s in shapes]
    else:
        shapes = [jax.ShapeDtypeStruct(*s) for s in shapes]
    return pl.pallas_call(
        body,
        out_shape=shapes,
        in_specs=[vmem] * count,
        out_specs=[vmem] * len(shapes),
        scratch_shapes=[pltpu.VMEM((entries, feats + 8, width), jnp.bfloat16)],
        name="products",
    )(*arrays)


def per_device(rows, cols, features, coeffs, targets):
    total = rows * cols
    core, xbit, z = cols, 2 * cols, 4 * cols
    f32, b16 = jnp.float32, jnp.bfloat16

    def swap(value, bits):
        return lax.ppermute(value, AXES, [(i, i ^ bits) for i in range(total)])

    mine = features.T
    outs = coeffs.shape[1]
    queries, order = [mine], [0]
    bit = rows // 8
    while bit >= 1:
        bits = bit * z
        queries = queries + [swap(q, bits) for q in queries]
        order = order + [o ^ bits for o in order]
        bit = bit // 2
    near = sum(a.size * a.dtype.itemsize for a in queries) * 8 <= NEAR_BYTES * 2
    both = stacked(coeffs.T, mine, near)
    queries[0] = both
    blocks = [both]
    for plane in reversed(range(1, 2 * cols)):
        bits = (plane // cols) * xbit + plane % cols
        blocks.append(swap(both, bits))
    keys = []
    for b in blocks:
        keys = keys + [b, swap(b, core)]

    feats = mine.shape[0]
    half = len(keys) // 2
    lead = queries[:-1] if len(queries) > 1 else queries
    run = functools.partial(products, outs=outs, feats=feats, near=near)
    got = run([(q, keys[:half], None) for q in lead], kinds=[f32] * len(lead), prepared=len(lead))
    early, ready = got[:len(lead)], [(a,) for a in got[len(lead):]]
    sent = [(q, keys[half:], e) for q, e in zip(ready, early)][1:]
    sent = sent + [(q, keys, None) for q in queries[len(lead):]]
    parts = run(sent, kinds=[b16] * len(sent)) if sent else []
    result = run([(ready[0], keys[half:], early[0])], kinds=[f32], minus=targets.T)[0]
    for n, part in enumerate(parts):
        result = result + swap(part, order[n + 1]).astype(f32)
    return result.T


def solution(mesh):
    rows, cols = mesh.shape["row"], mesh.shape["col"]
    spec = P(AXES, None)
    body = functools.partial(per_device, rows, cols)
    return jax.shard_map(
        body, mesh=mesh, in_specs=(spec, spec, spec), out_specs=spec, check_vma=False
    )
```

```python
import functools
import math

import jax
import jax.numpy as jnp
from jax import lax
from jax.experimental import pallas as pl
from jax.experimental.pallas import tpu as pltpu
from jax.sharding import PartitionSpec as P

AXES = ("row", "col")
NEAR_BYTES = 2 << 20
LOG2E = math.log2(math.e)


def square_rows(wide, shift):
    sq = jnp.sum(wide * wide, axis=0, keepdims=True)
    high = sq.astype(jnp.bfloat16).astype(jnp.float32)
    mid = (sq - high).astype(jnp.bfloat16).astype(jnp.float32)
    low = (sq - high) - mid
    row = lax.broadcasted_iota(jnp.int32, (8, wide.shape[1]), 0)
    rest = jnp.where(row < 6, 1.0, 0.0)
    for n, part in enumerate((high, mid, low)):
        rest = jnp.where(row == shift + n, part, rest)
    return rest.astype(jnp.bfloat16)


def stacked(weights, values, near):
    outs, feats, width = weights.shape[0], values.shape[0], values.shape[1]

    def body(weight_ref, value_ref, out_ref):
        out_ref[:outs, :] = weight_ref[...]
        value = value_ref[...]
        out_ref[outs:outs + feats, :] = value
        out_ref[outs + feats:, :] = square_rows(value.astype(jnp.float32), 0)

    shape = (outs + feats + 8, width)
    vmem = pl.BlockSpec(memory_space=pltpu.VMEM)
    return pl.pallas_call(
        body,
        out_shape=pltpu.VMEM(shape, values.dtype) if near else jax.ShapeDtypeStruct(shape, values.dtype),
        in_specs=[vmem] * 2,
        out_specs=vmem,
        name="stacked",
    )(weights, values)


def products(work, outs, feats, kinds, near, prepared=0, minus=None):
    arrays, slots = [], {}

    def slot(a):
        if id(a) not in slots:
            slots[id(a)] = len(arrays)
            arrays.append(a)
        return slots[id(a)]

    plan = [
        (
            slot(q[0] if isinstance(q, tuple) else q),
            isinstance(q, tuple),
            [slot(k) for k in keys],
            None if old is None else slot(old),
        )
        for q, keys, old in work
    ]
    taken = None if minus is None else slot(minus)
    count, entries = len(arrays), len(work)
    width = work[0][1][0].shape[1]

    def body(*refs):
        ins, out_refs, left_ref = refs[:count], refs[count:-1], refs[-1]
        lhs = []
        for n, (q, ready, _, _) in enumerate(plan):
            if ready:
                lhs.append(ins[q][...])
                continue
            skip = outs if ins[q].shape[0] > feats else 0
            wide = ins[q][skip:skip + feats, :].astype(jnp.float32)
            left_ref[n, :feats, :] = (wide * -2.0).astype(jnp.bfloat16)
            left_ref[n, feats:, :] = square_rows(wide, 3)
            lhs.append(left_ref[n].T)
        for n in range(prepared):
            out_refs[entries + n][...] = lhs[entries - prepared + n]
        acc = [None for _ in plan]
        groups = []
        for _, _, keys, _ in plan:
            for n in range(0, len(keys), 2):
                group = tuple(keys[n:n + 2])
                if group not in groups:
                    groups.append(group)
        for group in groups:
            rhs = jnp.concatenate([ins[k][outs:, :] for k in group], axis=1)
            weight = jnp.concatenate([ins[k][:outs, :] for k in group], axis=1)
            users = [i for i, (_, _, keys, _) in enumerate(plan) if group[0] in keys]
            left = jnp.concatenate([lhs[i] for i in users], axis=0)
            d2 = jnp.maximum(jnp.dot(left, rhs, preferred_element_type=jnp.float32), 1e-30)
            kern = jnp.exp2((d2 * -LOG2E) * lax.rsqrt(d2)).astype(jnp.bfloat16)
            part = lax.dot_general(
                kern, weight, (((1,), (1,)), ((), ())), preferred_element_type=jnp.float32
            )
            for n, i in enumerate(users):
                mine = part[n * width:(n + 1) * width, :]
                acc[i] = mine if acc[i] is None else acc[i] + mine
        for i in range(entries):
            total = acc[i].T
            old = plan[i][3]
            total = total if old is None else total + ins[old][...]
            total = total if taken is None else total - ins[taken][...]
            out_refs[i][...] = total.astype(out_refs[i].dtype)

    shapes = [((outs, width), kind) for kind in kinds]
    shapes = shapes + [((width, feats + 8), jnp.bfloat16)] * prepared
    vmem = pl.BlockSpec(memory_space=pltpu.VMEM)
    if near:
        arrays = [pltpu.with_memory_space_constraint(a, pltpu.VMEM) for a in arrays]
        shapes = [pltpu.VMEM(*s) for s in shapes]
    else:
        shapes = [jax.ShapeDtypeStruct(*s) for s in shapes]
    return pl.pallas_call(
        body,
        out_shape=shapes,
        in_specs=[vmem] * count,
        out_specs=[vmem] * len(shapes),
        scratch_shapes=[pltpu.VMEM((entries, feats + 8, width), jnp.bfloat16)],
        name="products",
    )(*arrays)


def per_device(rows, cols, features, coeffs, targets):
    total = rows * cols
    core, xbit, z = cols, 2 * cols, 4 * cols
    f32, b16 = jnp.float32, jnp.bfloat16

    def swap(value, bits):
        return lax.ppermute(value, AXES, [(i, i ^ bits) for i in range(total)])

    mine = features.T
    outs = coeffs.shape[1]
    queries, order = [mine], [0]
    bit = rows // 8
    while bit >= 1:
        bits = bit * z
        queries = queries + [swap(q, bits) for q in queries]
        order = order + [o ^ bits for o in order]
        bit = bit // 2
    near = sum(a.size * a.dtype.itemsize for a in queries) * 8 <= NEAR_BYTES * 2
    both = stacked(coeffs.T, mine, near)
    queries[0] = both
    blocks = [both]
    for plane in reversed(range(1, 2 * cols)):
        other = plane if plane == 2 * cols - 1 else 2 * cols - 1 - plane
        bits = [(p // cols) * xbit + p % cols for p in (plane, other)]
        pairs = [(i, i ^ bits[i // core % 2]) for i in range(total)]
        blocks.append(lax.ppermute(both, AXES, pairs))
    keys = []
    for b in blocks:
        keys = keys + [b, swap(b, core)]

    feats = mine.shape[0]
    half = len(keys) // 2
    lead = queries[:-1] if len(queries) > 1 else queries
    run = functools.partial(products, outs=outs, feats=feats, near=near)
    got = run([(q, keys[:half], None) for q in lead], kinds=[f32] * len(lead), prepared=len(lead))
    early, ready = got[:len(lead)], [(a,) for a in got[len(lead):]]
    sent = [(q, keys[half:], e) for q, e in zip(ready, early)][1:]
    sent = sent + [(q, keys, None) for q in queries[len(lead):]]
    parts = run(sent, kinds=[b16] * len(sent)) if sent else []
    result = run([(ready[0], keys[half:], early[0])], kinds=[f32], minus=targets.T)[0]
    for n, part in enumerate(parts):
        result = result + swap(part, order[n + 1]).astype(f32)
    return result.T


def solution(mesh):
    rows, cols = mesh.shape["row"], mesh.shape["col"]
    spec = P(AXES, None)
    body = functools.partial(per_device, rows, cols)
    return jax.shard_map(
        body, mesh=mesh, in_specs=(spec, spec, spec), out_specs=spec, check_vma=False
    )
```
